128 devices in a mesh: grp: 8 (over x_hi, y), mem: 16 (over z, x_lo, core).
Axes of the slice: x: 4 (x_hi: 2, x_lo: 2; x = x_hi * 2 + x_lo), y: 4, z: 4, core: 2. Of those that a mesh axis runs over, the one named last changes fastest.
Arguments:
- params: float32 [8, 2048, 2048], P('grp', 'mem'), may hold values from -6 to 6
- estimate: float32 [8, 2048, 2048], P('grp', 'mem'), may hold values from -6 to 6
- mixed_sum: float32 [8, 2048, 2048], P('grp', 'mem'), may hold values from -6 to 6
- activations: bfloat16 [131072, 2048], P(('grp', 'mem')), may hold values from -24 to 24
- out_grads: bfloat16 [131072, 2048], P(('grp', 'mem')), may hold values from -6 to 6
- exponents: int32 [8, 32], P('grp', 'mem'), may hold values from 0 to 3
- edge_weight: float32 [8], replicated, may hold values from 0.1 to 0.45
Outputs:
- new_params: float32 [8, 2048, 2048], P('grp', 'mem')
- new_estimate: float32 [8, 2048, 2048], P('grp', 'mem')
- new_mixed: float32 [8, 2048, 2048], P('grp', 'mem')
The draws below stay inside these ranges and needn't reach their ends.
All inputs are finite; a program needn't handle non-finite values.
Results may differ from the reference program's by a relative error of at most 0.01.
Values may be sent and summed in bfloat16 or wider, within the bound.
A program may use at most 128 MiB of HBM per device.

```python
import math
import jax
import jax.numpy as jnp
from jax import lax

D = 2048
INNER = 2048
TOK_DEV = 1024
BLOCK = 64
GROUPS = 8
ROWS = 131072
N_MEM = 16


def plant(entries, key, low, top_value):
    spot = [jax.random.randint(jax.random.fold_in(key, axis), (), 0, length) for axis, length in enumerate(entries.shape)]
    longest = entries.shape.index(max(entries.shape))
    neighbour = spot[:longest] + [(spot[longest] + 1) % entries.shape[longest]] + spot[longest + 1:]
    return entries.at[tuple(spot)].set(low).at[tuple(neighbour)].set(top_value)


def strengthened(array, stream_key, source, target, blocks, factor):
    def block_of(dim):
        return (jnp.arange(array.shape[dim]) // (array.shape[dim] // blocks)).reshape((-1,) + (1,) * (array.ndim - 1 - dim))

    first = jax.random.permutation(stream_key, blocks)[block_of(target)]
    second = (block_of(target) + blocks // 2) % blocks
    return jnp.where((block_of(source) == first) | (block_of(source) == second), factor * array, array)


def block_scale(stream_key, shape, cuts, smallest, largest):
    loudness, own = 1.0, jax.random.fold_in(stream_key, 6)
    for dim, shards_of in cuts:
        steps = jnp.exp(jax.random.uniform(jax.random.fold_in(own, dim), (shards_of,), jnp.float32, smallest / len(cuts), largest / len(cuts)))
        loudness = loudness * jnp.repeat(steps, shape[dim] // shards_of).reshape([-1 if axis == dim else 1 for axis in range(len(shape))])
    return loudness


def scatter_about(key, extent, scale, bound, pieces=(), dtype=jnp.bfloat16):
    drawn = jax.random.normal(key, extent, jnp.float32) * scale
    if len(pieces) > 0:
        drawn = block_scale(key, extent, pieces, -0.22, 0.18) * drawn
    return jnp.clip(drawn, min=-bound, max=bound).astype(dtype)


def gaussian_with(own_key, extent, spread, most, pieces, heavy, dtype=jnp.bfloat16):
    entries = spread * jax.random.normal(own_key, extent, jnp.float32)
    if pieces:
        entries = entries * block_scale(own_key, extent, pieces, -0.22, 0.18)
    return jnp.clip(strengthened(entries, jax.random.fold_in(own_key, 3), *heavy), -most, most).astype(dtype)


def setup_inputs(seed: int = 0) -> dict:
    key_list = jax.random.split(jax.random.key(seed), 8)
    params = scatter_about(key_list[0], (GROUPS, D, INNER), 1.0, 6.0, ((0, 8), (1, 16)), jnp.float32)
    estimate = scatter_about(key_list[1], (GROUPS, D, INNER), 1.0, 6.0, ((0, 8), (1, 16)), jnp.float32)
    mixed_sum = scatter_about(key_list[2], (GROUPS, D, INNER), 1.0, 6.0, ((0, 8), (1, 16)), jnp.float32)
    activations = gaussian_with(key_list[3], (ROWS, D), 1.0, 24.0, ((0, 128),), (0, 1, 128, 5.5))
    out_grads = scatter_about(key_list[4], (ROWS, INNER), 1.0, 6.0, ((0, 128),))
    exponents = plant(jax.random.randint(key_list[5], (GROUPS, D // BLOCK), 0, 4), jax.random.fold_in(key_list[5], 1), 0, 3).astype(jnp.int32)
    edge_weight = jnp.clip(jax.random.uniform(key_list[6], (GROUPS,), jnp.float32, 0.1, 0.45), 0.1, 0.45)
    return dict(params=params, estimate=estimate, mixed_sum=mixed_sum, activations=activations, out_grads=out_grads, exponents=exponents, edge_weight=edge_weight)


step_size = 0.5
mixing_rate = 0.4

def reference(params, estimate, mixed_sum, activations, out_grads, exponents, edge_weight):
    groups = params.shape[0]
    group_acts = activations.reshape(groups, N_MEM, TOK_DEV, D)
    group_outs = out_grads.reshape(groups, N_MEM, TOK_DEV, INNER)

    def group_gradient(blocks):

        def accumulate(running, member):
            partial_value = lax.dot_general(member[0], member[1], (((0,), (0,)), ((), ())), preferred_element_type=jnp.float32)
            rounded = lax.optimization_barrier(partial_value.astype(jnp.bfloat16))
            return (running + rounded.astype(jnp.float32), None)
        running, _ = lax.scan(accumulate, jnp.zeros((D, INNER), jnp.float32), blocks)
        return running
    gradient = lax.map(group_gradient, (group_acts, group_outs))
    factor = step_size / math.sqrt(N_MEM * TOK_DEV)
    stepped = params - factor * gradient
    change = stepped - estimate
    scales = jnp.exp2(exponents.astype(jnp.float32))[:, :, None, None]
    blocked = change.reshape(groups, D // BLOCK, BLOCK, INNER)
    levels = lax.optimization_barrier(jnp.clip(blocked / scales, -1.0, 1.0).astype(jnp.bfloat16))
    compressed = (levels.astype(jnp.float32) * scales).astype(jnp.bfloat16).reshape(groups, D, INNER)
    own_piece = compressed.astype(jnp.float32)
    new_estimate = estimate + own_piece
    left_piece = jnp.roll(compressed, 1, axis=0).astype(jnp.float32)
    right_piece = jnp.roll(compressed, -1, axis=0).astype(jnp.float32)
    weight_right = edge_weight
    weight_left = jnp.roll(edge_weight, 1)
    weight_self = 1.0 - weight_left - weight_right
    new_mixed = mixed_sum + weight_self[:, None, None] * own_piece
    new_mixed = new_mixed + weight_left[:, None, None] * left_piece
    new_mixed = new_mixed + weight_right[:, None, None] * right_piece
    new_params = stepped + mixing_rate * (new_mixed - new_estimate)
    return (new_params, new_estimate, new_mixed)
```

```python
import functools
import math

import jax
import jax.numpy as jnp
from jax import lax
from jax.experimental import pallas as pl
from jax.experimental.pallas import tpu as pltpu
from jax.sharding import PartitionSpec as P

step_size = 0.5
mixing_rate = 0.4

MESH = pl.DeviceIdType.MESH
F32 = jnp.float32
BF16 = jnp.bfloat16
CHUNKS = 8


def aligned(start, size):
    return pl.ds(pl.multiple_of(start, size), size)


def kernel(
    factor,
    params,
    estimate,
    mixed_sum,
    acts,
    grads,
    exponents,
    edge_weight,
    out_p,
    out_e,
    out_m,
    a_v,
    b_v,
    at_v,
    p_v,
    e_v,
    m_v,
    own_v,
    d_src,
    d_dst,
    near_v,
    home_v,
    s1_src,
    s1_dst,
    s2_src,
    s2_dst,
    x_src,
    x_dst,
    g_src,
    g_dst,
    a_sem,
    b_sem,
    l_sem,
    d_sem,
    s1_sem,
    s2_sem,
    x_sem,
    g_sem,
):
    g = lax.axis_index("grp")
    m = lax.axis_index("mem")
    z = m // 4
    x = (m // 2) % 2
    c = m % 2
    pc = 1 - c
    zp, zm, zo = (z + 1) % 4, (z + 3) % 4, (z + 2) % 4
    to_core = (g, z * 4 + x * 2 + pc)
    to_zp = (g, zp * 4 + x * 2 + c)
    to_zm = (g, zm * 4 + x * 2 + c)
    to_x = (g, z * 4 + (1 - x) * 2 + c)
    to_next = ((g + 1) % 8, m)
    to_prev = ((g + 7) % 8, m)
    chunks = CHUNKS
    cw = b_v.shape[2]

    barrier = pltpu.get_barrier_semaphore()
    for peer in (to_core, to_zp, to_zm, to_x, to_next, to_prev):
        pl.semaphore_signal(barrier, inc=1, device_id=peer, device_id_type=MESH)

    def load_a(par, q):
        return pltpu.make_async_copy(
            acts.at[:, aligned((2 * q + par) * 128, 128)], a_v.at[par, q], a_sem.at[par, q]
        )

    def load_b(k):
        return pltpu.make_async_copy(grads.at[:, aligned(k * cw, cw)], b_v.at[k], b_sem.at[k])

    def start_a(par):
        def body(q, _):
            load_a(par, q).start()
            return 0

        lax.fori_loop(0, 8, body, 0)

    start_a(pc)
    load_b(0).start()
    start_a(c)

    def start_b(k, _):
        load_b(k).start()
        return 0

    lax.fori_loop(1, chunks, start_b, 0)
    state = [
        pltpu.make_async_copy(src.at[0], dst, l_sem.at[i])
        for i, (src, dst) in enumerate(((params, p_v), (estimate, e_v), (mixed_sum, m_v)))
    ]
    for copy in state:
        copy.start()

    def transpose_a(par):
        def body(q, _):
            load_a(par, q).wait()
            at_v[par, aligned(q * 128, 128), :] = a_v[par, q].T
            return 0

        lax.fori_loop(0, 8, body, 0)

    def remote(src, dst, sems, index, peer):
        return pltpu.make_async_remote_copy(
            src_ref=src,
            dst_ref=dst,
            send_sem=sems.at[(0,) + index],
            recv_sem=sems.at[(1,) + index],
            device_id=peer,
            device_id_type=MESH,
        )

    def copy_d(k):
        return remote(d_src.at[k], d_dst.at[k], d_sem, (k,), to_core)

    def copy_s1(side, k):
        return remote(
            s1_src.at[side, k], s1_dst.at[side, k], s1_sem, (side, k), (to_zp, to_zm)[side]
        )

    def copy_s2(side, xd, k):
        return remote(
            s2_src.at[side, xd, k],
            s2_dst.at[side, xd, k],
            s2_sem,
            (side, xd, k),
            (to_zp, to_zm)[side],
        )

    def copy_x(k):
        return remote(x_src.at[k], x_dst.at[k], x_sem, (k,), to_x)

    def copy_g(side, k):
        return remote(g_src.at[k], g_dst.at[side, k], g_sem, (side, k), (to_next, to_prev)[side])

    def cols(k):
        return aligned(k * cw, cw)

    def multiply_partner(k):
        d_src[k] = jnp.dot(at_v[pc], b_v[k], preferred_element_type=F32).astype(BF16)
        copy_d(k).start()

    def multiply_own(k):
        own_v[k % 2] = jnp.dot(at_v[c], b_v[k], preferred_element_type=F32)

    def stage_a(k):
        load_b(k).wait()
        multiply_partner(k)
        multiply_own(k)

    def chip_sum(k, zd, xd):
        rows = aligned((zd * 2 + xd) * 128, 128)
        return own_v[k % 2, rows, :] + d_dst[k, rows, :].astype(F32)

    def stage_b(k):
        copy_d(k).wait_recv()
        for side in range(2):
            s1_src[side, k] = chip_sum(k, zo, side).astype(BF16)
            copy_s1(side, k).start()
        for side, zd in enumerate((zp, zm)):
            s2_src[side, 1 - side, k] = chip_sum(k, zd, 1 - side).astype(BF16)
            copy_s2(side, 1 - side, k).start()
        for side, zd in enumerate((zp, zm)):
            near_v[side, k] = chip_sum(k, zd, side)
        for xd in range(2):
            home_v[xd, k] = chip_sum(k, z, xd)

    def stage_c(k):
        for side in range(2):
            copy_s1(side, k).wait_recv()
            s2_src[side, side, k] = (near_v[side, k] + s1_dst[side, k].astype(F32)).astype(BF16)
            copy_s2(side, side, k).start()

    def line_sum(k, xd):
        return home_v[xd, k] + s2_dst[0, xd, k].astype(F32) + s2_dst[1, xd, k].astype(F32)

    def stage_d(k):
        for side in range(2):
            for xd in range(2):
                copy_s2(side, xd, k).wait_recv()
        x_src[k] = line_sum(k, 1 - x).astype(BF16)
        copy_x(k).start()
        home_v[x, k] = line_sum(k, x)

    w_right = edge_weight[g]
    w_left = edge_weight[(g + 7) % 8]
    w_self = 1.0 - w_left - w_right

    def stage_e(k):
        copy_x(k).wait_recv()
        gradient = home_v[x, k] + x_dst[k].astype(F32)
        old = e_v[:, cols(k)]
        stepped = p_v[:, cols(k)] - factor * gradient
        change = stepped - old
        parts = []
        for i in range(2):
            scale = jnp.full((64, cw), lax.shift_left(1, exponents[0, i]).astype(F32), F32)
            levels = jnp.clip(change[i * 64 : (i + 1) * 64] / scale, -1.0, 1.0).astype(BF16)
            parts.append((levels.astype(F32) * scale).astype(BF16))
        compressed = jnp.concatenate(parts, axis=0)
        g_src[k] = compressed
        for side in range(2):
            copy_g(side, k).start()
        piece = compressed.astype(F32)
        out_p[0, :, cols(k)] = stepped
        out_e[0, :, cols(k)] = old + piece
        out_m[0, :, cols(k)] = m_v[:, cols(k)] + w_self * piece

    def stage_f(k):
        for side in range(2):
            copy_g(side, k).wait_recv()
        mixed = out_m[0, :, cols(k)] + w_left * g_dst[0, k].astype(F32)
        mixed = mixed + w_right * g_dst[1, k].astype(F32)
        out_m[0, :, cols(k)] = mixed
        out_p[0, :, cols(k)] = out_p[0, :, cols(k)] + mixing_rate * (mixed - out_e[0, :, cols(k)])

    transpose_a(pc)
    load_b(0).wait()
    pl.semaphore_wait(barrier, 6)
    multiply_partner(0)
    transpose_a(c)
    multiply_own(0)
    for copy in state:
        copy.wait()

    def step(t, _):
        for stage, lag in (
            (stage_a, 0),
            (stage_b, 1),
            (stage_c, 2),
            (stage_d, 3),
            (stage_e, 4),
            (stage_f, 6),
        ):
            pl.when((t >= lag) & (t < chunks + lag))(functools.partial(stage, t - lag))
        return 0

    lax.fori_loop(1, chunks + 6, step, 0)

    def drain(k, _):
        copy_d(k).wait_send()
        copy_x(k).wait_send()
        for side in range(2):
            copy_s1(side, k).wait_send()
            copy_g(side, k).wait_send()
            for xd in range(2):
                copy_s2(side, xd, k).wait_send()
        return 0

    lax.fori_loop(0, chunks, drain, 0)


def on_device(params, estimate, mixed_sum, activations, out_grads, exponents, edge_weight):
    members = lax.axis_size("mem")
    tokens, width = out_grads.shape
    factor = step_size / math.sqrt(members * tokens)
    n = CHUNKS
    cw = width // n
    block = (128, cw)
    shard = jax.ShapeDtypeStruct(params.shape, F32)
    anywhere = pl.BlockSpec(memory_space=pl.ANY)
    vmem = pl.BlockSpec(memory_space=pltpu.VMEM)
    smem = pl.BlockSpec(memory_space=pltpu.SMEM)
    dma = pltpu.SemaphoreType.DMA
    return pl.pallas_call(
        functools.partial(kernel, factor),
        out_shape=(shard, shard, shard),
        in_specs=[anywhere] * 5 + [smem] * 2,
        out_specs=(vmem, vmem, vmem),
        scratch_shapes=[
            pltpu.VMEM((2, 8, tokens, 128), BF16),
            pltpu.VMEM((n, tokens, cw), BF16),
            pltpu.VMEM((2, 1024, tokens), BF16),
            pltpu.VMEM((128, width), F32),
            pltpu.VMEM((128, width), F32),
            pltpu.VMEM((128, width), F32),
            pltpu.VMEM((2, 1024, cw), F32),
            pltpu.VMEM((n, 1024, cw), BF16),
            pltpu.VMEM((n, 1024, cw), BF16),
            pltpu.VMEM((2, n) + block, F32),
            pltpu.VMEM((2, n) + block, F32),
            pltpu.VMEM((2, n) + block, BF16),
            pltpu.VMEM((2, n) + block, BF16),
            pltpu.VMEM((2, 2, n) + block, BF16),
            pltpu.VMEM((2, 2, n) + block, BF16),
            pltpu.VMEM((n,) + block, BF16),
            pltpu.VMEM((n,) + block, BF16),
            pltpu.VMEM((n,) + block, BF16),
            pltpu.VMEM((2, n) + block, BF16),
            dma((2, 8)),
            dma((n,)),
            dma((3,)),
            dma((2, n)),
            dma((2, 2, n)),
            dma((2, 2, 2, n)),
            dma((2, n)),
            dma((2, 2, n)),
        ],
        compiler_params=pltpu.CompilerParams(
            collective_id=0, has_side_effects=True, vmem_limit_bytes=50 * 2**20
        ),
        name="round",
    )(params, estimate, mixed_sum, activations, out_grads, exponents, edge_weight)


def solution(mesh):
    in_specs = (
        P("grp", "mem", None),
        P("grp", "mem", None),
        P("grp", "mem", None),
        P(("grp", "mem"), None),
        P(("grp", "mem"), None),
        P("grp", "mem"),
        P(),
    )
    out_specs = (P("grp", "mem", None), P("grp", "mem", None), P("grp", "mem", None))
    return jax.shard_map(
        on_device, mesh=mesh, in_specs=in_specs, out_specs=out_specs, check_vma=False
    )
```

```python
import functools
import math

import jax
import jax.numpy as jnp
from jax import lax
from jax.experimental import pallas as pl
from jax.experimental.pallas import tpu as pltpu
from jax.sharding import PartitionSpec as P

step_size = 0.5
mixing_rate = 0.4

MESH = pl.DeviceIdType.MESH
F32 = jnp.float32
BF16 = jnp.bfloat16
CHUNKS = 8
WIDE = 2
HEAD = 2


def aligned(start, size):
    return pl.ds(pl.multiple_of(start, size), size)


def kernel(
    factor,
    params,
    estimate,
    mixed_sum,
    acts,
    grads,
    exponents,
    edge_weight,
    out_p,
    out_e,
    out_m,
    a_v,
    b_v,
    at_v,
    p_v,
    e_v,
    m_v,
    own_v,
    d_src,
    d_dst,
    near_v,
    home_v,
    s1_src,
    s1_dst,
    s2_src,
    s2_dst,
    x_src,
    x_dst,
    wide_own,
    wide_src,
    wide_dst,
    near_w,
    home_w,
    w1_src,
    w1_dst,
    w2_src,
    w2_dst,
    g_src,
    g_dst,
    h_src,
    h_dst,
    powers,
    weights,
    a_sem,
    b_sem,
    l_sem,
    d_sem,
    head_sem,
    s1_sem,
    s2_sem,
    x_sem,
    wide_sem,
    w1_sem,
    w2_sem,
    g_sem,
    h_sem,
):
    g = lax.axis_index("grp")
    m = lax.axis_index("mem")
    z = m // 4
    x = (m // 2) % 2
    c = m % 2
    pc = 1 - c
    zp, zm, zo = (z + 1) % 4, (z + 3) % 4, (z + 2) % 4
    to_core = (g, z * 4 + x * 2 + pc)
    to_line = ((g, zp * 4 + x * 2 + c), (g, zm * 4 + x * 2 + c))
    to_x = (g, z * 4 + (1 - x) * 2 + c)
    to_cycle = (((g + 1) % 8, m), ((g + 7) % 8, m))
    chunks, _, cw = b_v.shape
    pieces, _, _, pw = wide_src.shape
    wide = pieces * pw // cw
    slim = chunks - wide
    line = (zo, zp, zm, z)

    barrier = pltpu.get_barrier_semaphore()
    for peer in (to_core, to_x) + to_line + to_cycle:
        pl.semaphore_signal(barrier, inc=1, device_id=peer, device_id_type=MESH)

    def load_a(i, slot):
        j, xd, par = i
        block = line[j] * 4 + xd * 2 + (pc, c)[par]
        return pltpu.make_async_copy(
            acts.at[:, aligned(block * 128, 128)], a_v.at[slot], a_sem.at[slot]
        )

    def load_b(k):
        return pltpu.make_async_copy(grads.at[:, aligned(k * cw, cw)], b_v.at[k], b_sem.at[k])

    blocks = [(0, xd, par) for par in range(2) for xd in range(2)]
    blocks += [(j, xd, par) for par in range(2) for j in range(1, 4) for xd in range(2)]
    for slot, i in enumerate(blocks):
        if slot == 4:
            for k in range(HEAD):
                load_b(k).start()
        load_a(i, slot).start()
    small = [
        pltpu.make_async_copy(exponents, powers, l_sem.at[3]),
        pltpu.make_async_copy(edge_weight, weights, l_sem.at[4]),
    ]
    state = [
        pltpu.make_async_copy(src.at[0], dst, l_sem.at[i])
        for i, (src, dst) in enumerate(((params, p_v), (estimate, e_v), (mixed_sum, m_v)))
    ]
    for k in (slim, HEAD, *range(slim + 1, chunks), *range(HEAD + 1, slim)):
        load_b(k).start()
    for copy in small + state:
        copy.start()

    def transpose_a(low, high):
        def body(slot, _):
            pltpu.make_async_copy(
                acts.at[:, pl.ds(0, 128)], a_v.at[slot], a_sem.at[slot]
            ).wait()
            at_v[aligned(slot * 128, 128), :] = a_v[slot].T
            return 0

        lax.fori_loop(low, high, body, 0)

    def remote(src, dst, sems, index, peer):
        return pltpu.make_async_remote_copy(
            src_ref=src,
            dst_ref=dst,
            send_sem=sems.at[(0,) + index],
            recv_sem=sems.at[(1,) + index],
            device_id=peer,
            device_id_type=MESH,
        )

    def copy_d(k):
        return remote(d_src.at[k], d_dst.at[k], d_sem, (k,), to_core)

    def copy_head(k):
        rows = pl.ds(0, 256)
        return remote(d_src.at[k, rows], d_dst.at[k, rows], head_sem, (k,), to_core)

    def copy_rest(k):
        rows = pl.ds(256, 768)
        return remote(d_src.at[k, rows], d_dst.at[k, rows], d_sem, (k,), to_core)

    def copy_s1(side, k):
        return remote(
            s1_src.at[side, k], s1_dst.at[side, k], s1_sem, (side, k), to_line[side]
        )

    def copy_s2(side, xd, k):
        return remote(
            s2_src.at[side, xd, k],
            s2_dst.at[side, xd, k],
            s2_sem,
            (side, xd, k),
            to_line[side],
        )

    def copy_x(k):
        return remote(x_src.at[k], x_dst.at[k], x_sem, (k,), to_x)

    def copy_wide(i):
        return remote(wide_src.at[i], wide_dst.at[i], wide_sem, (i,), to_x)

    def copy_w1(side, i):
        return remote(
            w1_src.at[side, i], w1_dst.at[side, i], w1_sem, (side, i), to_line[side]
        )

    def copy_w2(side, half, i):
        return remote(
            w2_src.at[side, half, i],
            w2_dst.at[side, half, i],
            w2_sem,
            (side, half, i),
            to_line[side],
        )

    def copy_g(side, k):
        return remote(
            g_src.at[k], g_dst.at[side, k], g_sem, (side, k), to_cycle[side]
        )

    def copy_h(side, i):
        return remote(
            h_src.at[i], h_dst.at[side, i], h_sem, (side, i), to_cycle[side]
        )

    def multiply(k, slot):
        load_b(k).wait()
        both = jnp.dot(at_v[...], b_v[k], preferred_element_type=F32)
        d_src[k, pl.ds(0, 256), :] = both[:256].astype(BF16)
        own_v[slot, pl.ds(0, 256), :] = both[256:512]
        d_src[k, pl.ds(256, 768), :] = both[512:1280].astype(BF16)
        own_v[slot, pl.ds(256, 768), :] = both[1280:]
        copy_d(k).start()

    def multiply_head(k, _):
        load_b(k).wait()
        both = jnp.dot(at_v[pl.ds(0, 512), :], b_v[k], preferred_element_type=F32)
        d_src[k, pl.ds(0, 256), :] = both[:256].astype(BF16)
        own_v[k, pl.ds(0, 256), :] = both[256:]
        return 0

    def multiply_rest(k, _):
        both = jnp.dot(at_v[pl.ds(512, 1536), :], b_v[k], preferred_element_type=F32)
        d_src[k, pl.ds(256, 768), :] = both[:768].astype(BF16)
        own_v[k, pl.ds(256, 768), :] = both[768:]
        copy_rest(k).start()
        return 0

    def slim_multiply(k):
        multiply(k, k % 2)

    def wide_multiply(i):
        multiply(slim + i, 2 + i)

    def chip_sum(k, slot, j, xd):
        rows = aligned((j * 2 + xd) * 128, 128)
        return own_v[slot, rows, :] + d_dst[k, rows, :].astype(F32)

    def send_first(k):
        for side in range(2):
            s1_src[side, k] = chip_sum(k, k % 2, 0, side).astype(BF16)
            copy_s1(side, k).start()

    def send_direct(k):
        part = functools.partial(chip_sum, k, k % 2)
        for side in range(2):
            s2_src[side, 1 - side, k] = part(1 + side, 1 - side).astype(BF16)
            copy_s2(side, 1 - side, k).start()
        for side in range(2):
            near_v[side, k] = part(1 + side, side)
        for xd in range(2):
            home_v[xd, k] = part(3, xd)

    def head_first(k):
        copy_head(k).wait_recv()
        send_first(k)

    def head_direct(k):
        copy_rest(k).wait_recv()
        send_direct(k)

    def slim_first(k):
        k = k + HEAD
        copy_d(k).wait_recv()
        send_first(k)
        send_direct(k)

    def slim_relay(k):
        for side in range(2):
            copy_s1(side, k).wait_recv()
            s2_src[side, side, k] = (near_v[side, k] + s1_dst[side, k].astype(F32)).astype(BF16)
            copy_s2(side, side, k).start()

    def slim_cross(k):
        for side in range(2):
            for xd in range(2):
                copy_s2(side, xd, k).wait_recv()

        def line_sum(xd):
            return home_v[xd, k] + s2_dst[0, xd, k].astype(F32) + s2_dst[1, xd, k].astype(F32)

        x_src[k] = line_sum(1 - x).astype(BF16)
        copy_x(k).start()
        home_v[x, k] = line_sum(x)

    def slim_finish(k):
        copy_x(k).wait_recv()
        compress(aligned(k * cw, cw), home_v[x, k] + x_dst[k].astype(F32), g_src.at[k])
        for side in range(2):
            copy_g(side, k).start()

    def wide_first(i):
        k = slim + i
        copy_d(k).wait_recv()
        for j in range(4):
            away = chip_sum(k, 2 + i, j, 1 - x).astype(BF16)
            for part in range(cw // pw):
                wide_src[i * (cw // pw) + part, j] = away[:, part * pw : (part + 1) * pw]
        for part in range(cw // pw):
            copy_wide(i * (cw // pw) + part).start()
        for j in range(4):
            keep = chip_sum(k, 2 + i, j, x)
            for part in range(cw // pw):
                wide_own[i * (cw // pw) + part, j] = keep[:, part * pw : (part + 1) * pw]

    def wide_line(i):
        copy_wide(i).wait_recv()

        def pair_sum(j, half):
            rows = pl.ds(half * 64, 64)
            return wide_own[i, j, rows, :] + wide_dst[i, j, rows, :].astype(F32)

        for side in range(2):
            w1_src[side, i] = pair_sum(0, side).astype(BF16)
            copy_w1(side, i).start()
        for side in range(2):
            w2_src[side, 1 - side, i] = pair_sum(1 + side, 1 - side).astype(BF16)
            copy_w2(side, 1 - side, i).start()
        for side in range(2):
            near_w[side, i] = pair_sum(1 + side, side)
        for half in range(2):
            home_w[half, i] = pair_sum(3, half)

    def wide_relay(i):
        for side in range(2):
            copy_w1(side, i).wait_recv()
            w2_src[side, side, i] = (near_w[side, i] + w1_dst[side, i].astype(F32)).astype(BF16)
            copy_w2(side, side, i).start()

    def wide_finish(i):
        for side in range(2):
            for half in range(2):
                copy_w2(side, half, i).wait_recv()
        sums = [
            home_w[half, i] + w2_dst[0, half, i].astype(F32) + w2_dst[1, half, i].astype(F32)
            for half in range(2)
        ]
        start = slim * cw + i * pw
        compress(aligned(start, pw), jnp.concatenate(sums, axis=0), h_src.at[i])
        for side in range(2):
            copy_h(side, i).start()

    for copy in small:
        copy.wait()
    w_right = weights[g]
    w_left = weights[(g + 7) % 8]
    w_self = 1.0 - w_left - w_right

    def compress(cols, gradient, sent):
        old = e_v[:, cols]
        stepped = p_v[:, cols] - factor * gradient
        change = stepped - old
        parts = []
        for i in range(2):
            scale = lax.shift_left(1, powers[0, i]).astype(F32)
            scale = jnp.full((64, change.shape[1]), scale, F32)
            levels = jnp.clip(change[i * 64 : (i + 1) * 64] / scale, -1.0, 1.0).astype(BF16)
            parts.append((levels.astype(F32) * scale).astype(BF16))
        compressed = jnp.concatenate(parts, axis=0)
        sent[...] = compressed
        piece = compressed.astype(F32)
        out_p[0, :, cols] = stepped
        out_e[0, :, cols] = old + piece
        out_m[0, :, cols] = m_v[:, cols] + w_self * piece

    def mix(cols, left, right):
        mixed = out_m[0, :, cols] + w_left * left[...].astype(F32)
        mixed = mixed + w_right * right[...].astype(F32)
        out_m[0, :, cols] = mixed
        out_p[0, :, cols] = out_p[0, :, cols] + mixing_rate * (mixed - out_e[0, :, cols])

    def slim_mix(k):
        for side in range(2):
            copy_g(side, k).wait_recv()
        mix(aligned(k * cw, cw), g_dst.at[0, k], g_dst.at[1, k])

    def wide_mix(i):
        for side in range(2):
            copy_h(side, i).wait_recv()
        mix(aligned(slim * cw + i * pw, pw), h_dst.at[0, i], h_dst.at[1, i])

    transpose_a(0, 4)
    lax.fori_loop(0, HEAD, multiply_head, 0)
    pl.semaphore_wait(barrier, 6)
    for k in range(HEAD):
        copy_head(k).start()
    transpose_a(4, 16)
    for k in range(HEAD):
        head_first(k)
    lax.fori_loop(0, HEAD, multiply_rest, 0)
    for copy in state:
        copy.wait()

    def step(t, _):
        for stage, lag, count in (
            (head_direct, 0, HEAD),
            (slim_first, HEAD, slim - HEAD),
            (wide_line, 4, pieces),
            (slim_relay, 1, slim),
            (wide_relay, 6, pieces),
            (lambda i: slim_multiply(i + HEAD), 1, slim - HEAD),
            (wide_multiply, 0, wide),
            (wide_first, 1, wide),
            (slim_cross, 3, slim),
            (wide_finish, 8, pieces),
            (slim_finish, 4, slim),
            (slim_mix, 7, slim),
            (wide_mix, 11, pieces),
        ):
            pl.when((t >= lag) & (t < count + lag))(functools.partial(stage, t - lag))
        return 0

    lax.fori_loop(0, 15, step, 0)

    def drain_slim(k, _):
        copy_x(k).wait_send()
        for side in range(2):
            copy_g(side, k).wait_send()
            copy_s1(side, k).wait_send()
            for xd in range(2):
                copy_s2(side, xd, k).wait_send()
        return 0

    def drain_wide(i, _):
        copy_wide(i).wait_send()
        for side in range(2):
            copy_h(side, i).wait_send()
            copy_w1(side, i).wait_send()
            for half in range(2):
                copy_w2(side, half, i).wait_send()
        return 0

    def drain_head(k, _):
        copy_head(k).wait_send()
        copy_rest(k).wait_send()
        return 0

    def drain(k, _):
        copy_d(k).wait_send()
        return 0

    lax.fori_loop(0, slim, drain_slim, 0)
    lax.fori_loop(0, pieces, drain_wide, 0)
    lax.fori_loop(0, HEAD, drain_head, 0)
    lax.fori_loop(HEAD, chunks, drain, 0)


def store(in_p, in_e, in_m, out_p, out_e, out_m, sems):
    copies = [
        pltpu.make_async_copy(src, dst, sems.at[i])
        for i, (src, dst) in enumerate(((in_p, out_p), (in_e, out_e), (in_m, out_m)))
    ]
    for copy in copies:
        copy.start()
    for copy in copies:
        copy.wait()


def on_device(params, estimate, mixed_sum, activations, out_grads, exponents, edge_weight):
    members = lax.axis_size("mem")
    tokens, width = out_grads.shape
    factor = step_size / math.sqrt(members * tokens)
    n = CHUNKS
    cw = width // n
    w = WIDE
    r = n - w
    p = w * cw // 128
    block = (128, cw)
    piece = (128, 128)
    half = (64, 128)
    shard = jax.ShapeDtypeStruct(params.shape, F32)
    anywhere = pl.BlockSpec(memory_space=pl.ANY)
    hbm = pl.BlockSpec(memory_space=pltpu.HBM)
    vmem = pl.BlockSpec(memory_space=pltpu.VMEM)
    dma = pltpu.SemaphoreType.DMA
    exponents = pltpu.with_memory_space_constraint(exponents, pltpu.HBM)
    edge_weight = pltpu.with_memory_space_constraint(edge_weight, pltpu.HBM)
    results = pl.pallas_call(
        functools.partial(kernel, factor),
        out_shape=(shard, shard, shard),
        in_specs=[hbm] * 7,
        out_specs=(vmem, vmem, vmem),
        scratch_shapes=[
            pltpu.VMEM((16, tokens, 128), BF16),
            pltpu.VMEM((n, tokens, cw), BF16),
            pltpu.VMEM((2048, tokens), BF16),
            pltpu.VMEM((128, width), F32),
            pltpu.VMEM((128, width), F32),
            pltpu.VMEM((128, width), F32),
            pltpu.VMEM((2 + w, 1024, cw), F32),
            pltpu.VMEM((n, 1024, cw), BF16),
            pltpu.VMEM((n, 1024, cw), BF16),
            pltpu.VMEM((2, r) + block, F32),
            pltpu.VMEM((2, r) + block, F32),
            pltpu.VMEM((2, r) + block, BF16),
            pltpu.VMEM((2, r) + block, BF16),
            pltpu.VMEM((2, 2, r) + block, BF16),
            pltpu.VMEM((2, 2, r) + block, BF16),
            pltpu.VMEM((r,) + block, BF16),
            pltpu.VMEM((r,) + block, BF16),
            pltpu.VMEM((p, 4) + piece, F32),
            pltpu.VMEM((p, 4) + piece, BF16),
            pltpu.VMEM((p, 4) + piece, BF16),
            pltpu.VMEM((2, p) + half, F32),
            pltpu.VMEM((2, p) + half, F32),
            pltpu.VMEM((2, p) + half, BF16),
            pltpu.VMEM((2, p) + half, BF16),
            pltpu.VMEM((2, 2, p) + half, BF16),
            pltpu.VMEM((2, 2, p) + half, BF16),
            pltpu.VMEM((r,) + block, BF16),
            pltpu.VMEM((2, r) + block, BF16),
            pltpu.VMEM((p,) + piece, BF16),
            pltpu.VMEM((2, p) + piece, BF16),
            pltpu.SMEM((1, 2), jnp.int32),
            pltpu.SMEM((8,), F32),
            dma((16,)),
            dma((n,)),
            dma((5,)),
            dma((2, n)),
            dma((2, HEAD)),
            dma((2, 2, r)),
            dma((2, 2, 2, r)),
            dma((2, r)),
            dma((2, p)),
            dma((2, 2, p)),
            dma((2, 2, 2, p)),
            dma((2, 2, r)),
            dma((2, 2, p)),
        ],
        compiler_params=pltpu.CompilerParams(
            collective_id=0, has_side_effects=True, vmem_limit_bytes=50 * 2**20
        ),
        name="round",
    )(params, estimate, mixed_sum, activations, out_grads, exponents, edge_weight)
    return pl.pallas_call(
        store,
        out_shape=(shard, shard, shard),
        in_specs=[vmem] * 3,
        out_specs=(anywhere,) * 3,
        scratch_shapes=[dma((3,))],
        compiler_params=pltpu.CompilerParams(vmem_limit_bytes=2**20),
        name="store",
    )(*results)


def solution(mesh):
    in_specs = (
        P("grp", "mem", None),
        P("grp", "mem", None),
        P("grp", "mem", None),
        P(("grp", "mem"), None),
        P(("grp", "mem"), None),
        P("grp", "mem"),
        P(),
    )
    out_specs = (P("grp", "mem", None), P("grp", "mem", None), P("grp", "mem", None))
    return jax.shard_map(
        on_device, mesh=mesh, in_specs=in_specs, out_specs=out_specs, check_vma=False
    )
```

```python
import functools
import math

import jax
import jax.numpy as jnp
from jax import lax
from jax.experimental import pallas as pl
from jax.experimental.pallas import tpu as pltpu
from jax.sharding import PartitionSpec as P

step_size = 0.5
mixing_rate = 0.4

MESH = pl.DeviceIdType.MESH
F32 = jnp.float32
BF16 = jnp.bfloat16
CHUNKS = 8
WIDE = 2
HEAD = 2


def aligned(start, size):
    return pl.ds(pl.multiple_of(start, size), size)


def kernel(
    factor,
    params,
    estimate,
    mixed_sum,
    acts,
    grads,
    exponents,
    edge_weight,
    out_p,
    out_e,
    out_m,
    a_v,
    b_v,
    at_v,
    p_v,
    e_v,
    m_v,
    own_v,
    d_src,
    d_dst,
    near_v,
    home_v,
    s1_src,
    s1_dst,
    s2_src,
    s2_dst,
    x_src,
    x_dst,
    wide_own,
    wide_src,
    wide_dst,
    near_w,
    home_w,
    w1_src,
    w1_dst,
    w2_src,
    w2_dst,
    g_src,
    g_dst,
    h_src,
    h_dst,
    powers,
    weights,
    a_sem,
    b_sem,
    l_sem,
    d_sem,
    head_sem,
    s1_sem,
    s2_sem,
    x_sem,
    wide_sem,
    w1_sem,
    w2_sem,
    g_sem,
    h_sem,
):
    g = lax.axis_index("grp")
    m = lax.axis_index("mem")
    z = m // 4
    x = (m // 2) % 2
    c = m % 2
    pc = 1 - c
    zp, zm, zo = (z + 1) % 4, (z + 3) % 4, (z + 2) % 4
    to_core = (g, z * 4 + x * 2 + pc)
    to_line = ((g, zp * 4 + x * 2 + c), (g, zm * 4 + x * 2 + c))
    to_x = (g, z * 4 + (1 - x) * 2 + c)
    to_cycle = (((g + 1) % 8, m), ((g + 7) % 8, m))
    chunks, _, cw = b_v.shape
    pieces, _, _, pw = wide_src.shape
    wide = pieces * pw // cw
    slim = chunks - wide
    line = (zo, zp, zm, z)

    barrier = pltpu.get_barrier_semaphore()
    for peer in (to_core, to_x) + to_line + to_cycle:
        pl.semaphore_signal(barrier, inc=1, device_id=peer, device_id_type=MESH)

    def load_a(i, slot):
        j, xd, par = i
        block = line[j] * 4 + xd * 2 + (pc, c)[par]
        return pltpu.make_async_copy(
            acts.at[:, aligned(block * 128, 128)], a_v.at[slot], a_sem.at[slot]
        )

    def load_b(k):
        return pltpu.make_async_copy(grads.at[:, aligned(k * cw, cw)], b_v.at[k], b_sem.at[k])

    blocks = [(0, xd, par) for par in range(2) for xd in range(2)]
    blocks += [(j, xd, par) for par in range(2) for j in range(1, 4) for xd in range(2)]
    for slot, i in enumerate(blocks):
        if slot == 4:
            for k in range(HEAD):
                load_b(k).start()
        load_a(i, slot).start()
    small = [
        pltpu.make_async_copy(exponents, powers, l_sem.at[3]),
        pltpu.make_async_copy(edge_weight, weights, l_sem.at[4]),
    ]
    state = [
        pltpu.make_async_copy(src.at[0], dst, l_sem.at[i])
        for i, (src, dst) in enumerate(((params, p_v), (estimate, e_v), (mixed_sum, m_v)))
    ]
    for k in (slim, HEAD, *range(slim + 1, chunks), *range(HEAD + 1, slim)):
        load_b(k).start()
    for copy in small + state:
        copy.start()

    def transpose_a(low, high):
        def body(slot, _):
            pltpu.make_async_copy(
                acts.at[:, pl.ds(0, 128)], a_v.at[slot], a_sem.at[slot]
            ).wait()
            at_v[aligned(slot * 128, 128), :] = a_v[slot].T
            return 0

        lax.fori_loop(low, high, body, 0)

    def remote(src, dst, sems, index, peer):
        return pltpu.make_async_remote_copy(
            src_ref=src,
            dst_ref=dst,
            send_sem=sems.at[(0,) + index],
            recv_sem=sems.at[(1,) + index],
            device_id=peer,
            device_id_type=MESH,
        )

    def copy_d(k):
        return remote(d_src.at[k], d_dst.at[k], d_sem, (k,), to_core)

    def copy_head(k):
        rows = pl.ds(0, 256)
        return remote(d_src.at[k, rows], d_dst.at[k, rows], head_sem, (k,), to_core)

    def copy_rest(k):
        rows = pl.ds(256, 768)
        return remote(d_src.at[k, rows], d_dst.at[k, rows], d_sem, (k,), to_core)

    def copy_s1(side, k):
        return remote(
            s1_src.at[side, k], s1_dst.at[side, k], s1_sem, (side, k), to_line[side]
        )

    def copy_s2(side, xd, k):
        return remote(
            s2_src.at[side, xd, k],
            s2_dst.at[side, xd, k],
            s2_sem,
            (side, xd, k),
            to_line[side],
        )

    def copy_x(k):
        return remote(x_src.at[k], x_dst.at[k], x_sem, (k,), to_x)

    def copy_wide(i):
        return remote(wide_src.at[i], wide_dst.at[i], wide_sem, (i,), to_x)

    def copy_w1(side, i):
        return remote(
            w1_src.at[side, i], w1_dst.at[side, i], w1_sem, (side, i), to_line[side]
        )

    def copy_w2(side, half, i):
        return remote(
            w2_src.at[side, half, i],
            w2_dst.at[side, half, i],
            w2_sem,
            (side, half, i),
            to_line[side],
        )

    def copy_g(side, k):
        return remote(
            g_src.at[k], g_dst.at[side, k], g_sem, (side, k), to_cycle[side]
        )

    def copy_h(side, i):
        return remote(
            h_src.at[i], h_dst.at[side, i], h_sem, (side, i), to_cycle[side]
        )

    def multiply(k, slot):
        load_b(k).wait()
        both = jnp.dot(at_v[...], b_v[k], preferred_element_type=F32)
        d_src[k, pl.ds(0, 256), :] = both[:256].astype(BF16)
        own_v[slot, pl.ds(0, 256), :] = both[256:512]
        d_src[k, pl.ds(256, 768), :] = both[512:1280].astype(BF16)
        own_v[slot, pl.ds(256, 768), :] = both[1280:]
        copy_d(k).start()

    def multiply_head(k, _):
        load_b(k).wait()
        both = jnp.dot(at_v[pl.ds(0, 512), :], b_v[k], preferred_element_type=F32)
        d_src[k, pl.ds(0, 256), :] = both[:256].astype(BF16)
        own_v[k, pl.ds(0, 256), :] = both[256:]
        return 0

    def multiply_rest(k, _):
        both = jnp.dot(at_v[pl.ds(512, 1536), :], b_v[k], preferred_element_type=F32)
        d_src[k, pl.ds(256, 768), :] = both[:768].astype(BF16)
        own_v[k, pl.ds(256, 768), :] = both[768:]
        copy_rest(k).start()
        return 0

    def slim_multiply(k):
        multiply(k, k % 2)

    def wide_multiply(i):
        multiply(slim + i, 2 + i)

    def chip_sum(k, slot, j, xd):
        rows = aligned((j * 2 + xd) * 128, 128)
        return own_v[slot, rows, :] + d_dst[k, rows, :].astype(F32)

    def send_first(k):
        for side in range(2):
            s1_src[side, k] = chip_sum(k, k % 2, 0, side).astype(BF16)
            copy_s1(side, k).start()

    def send_direct(k):
        part = functools.partial(chip_sum, k, k % 2)
        for side in range(2):
            s2_src[side, 1 - side, k] = part(1 + side, 1 - side).astype(BF16)
            copy_s2(side, 1 - side, k).start()
        for side in range(2):
            near_v[side, k] = part(1 + side, side)
        for xd in range(2):
            home_v[xd, k] = part(3, xd)

    def head_first(k):
        copy_head(k).wait_recv()
        send_first(k)

    def head_direct(k):
        copy_rest(k).wait_recv()
        send_direct(k)

    def slim_first(k):
        k = k + HEAD
        copy_d(k).wait_recv()
        send_first(k)
        send_direct(k)

    def slim_relay(k):
        for side in range(2):
            copy_s1(side, k).wait_recv()
            s2_src[side, side, k] = (near_v[side, k] + s1_dst[side, k].astype(F32)).astype(BF16)
            copy_s2(side, side, k).start()

    def slim_cross(k):
        for side in range(2):
            for xd in range(2):
                copy_s2(side, xd, k).wait_recv()

        def line_sum(xd):
            return home_v[xd, k] + s2_dst[0, xd, k].astype(F32) + s2_dst[1, xd, k].astype(F32)

        x_src[k] = line_sum(1 - x).astype(BF16)
        copy_x(k).start()
        home_v[x, k] = line_sum(x)

    def slim_finish(k):
        copy_x(k).wait_recv()
        compress(aligned(k * cw, cw), home_v[x, k] + x_dst[k].astype(F32), g_src.at[k])
        for side in range(2):
            copy_g(side, k).start()

    def wide_first(i):
        k = slim + i
        copy_d(k).wait_recv()
        for j in range(4):
            away = chip_sum(k, 2 + i, j, 1 - x).astype(BF16)
            for part in range(cw // pw):
                wide_src[i * (cw // pw) + part, j] = away[:, part * pw : (part + 1) * pw]
        for part in range(cw // pw):
            copy_wide(i * (cw // pw) + part).start()
        for j in range(4):
            keep = chip_sum(k, 2 + i, j, x)
            for part in range(cw // pw):
                wide_own[i * (cw // pw) + part, j] = keep[:, part * pw : (part + 1) * pw]

    def wide_line(i):
        copy_wide(i).wait_recv()

        def pair_sum(j, half):
            rows = pl.ds(half * 64, 64)
            return wide_own[i, j, rows, :] + wide_dst[i, j, rows, :].astype(F32)

        for side in range(2):
            w1_src[side, i] = pair_sum(0, side).astype(BF16)
            copy_w1(side, i).start()
        for side in range(2):
            w2_src[side, 1 - side, i] = pair_sum(1 + side, 1 - side).astype(BF16)
            copy_w2(side, 1 - side, i).start()
        for side in range(2):
            near_w[side, i] = pair_sum(1 + side, side)
        for half in range(2):
            home_w[half, i] = pair_sum(3, half)

    def wide_relay(i):
        for side in range(2):
            copy_w1(side, i).wait_recv()
            w2_src[side, side, i] = (near_w[side, i] + w1_dst[side, i].astype(F32)).astype(BF16)
            copy_w2(side, side, i).start()

    def wide_finish(i):
        for side in range(2):
            for half in range(2):
                copy_w2(side, half, i).wait_recv()
        sums = [
            home_w[half, i] + w2_dst[0, half, i].astype(F32) + w2_dst[1, half, i].astype(F32)
            for half in range(2)
        ]
        start = slim * cw + i * pw
        compress(aligned(start, pw), jnp.concatenate(sums, axis=0), h_src.at[i])
        for side in range(2):
            copy_h(side, i).start()

    for copy in small:
        copy.wait()
    w_right = weights[g]
    w_left = weights[(g + 7) % 8]
    w_self = 1.0 - w_left - w_right

    def compress(cols, gradient, sent):
        old = e_v[:, cols]
        stepped = p_v[:, cols] - factor * gradient
        change = stepped - old
        parts = []
        for i in range(2):
            scale = lax.shift_left(1, powers[0, i]).astype(F32)
            scale = jnp.full((64, change.shape[1]), scale, F32)
            levels = jnp.clip(change[i * 64 : (i + 1) * 64] / scale, -1.0, 1.0).astype(BF16)
            parts.append((levels.astype(F32) * scale).astype(BF16))
        compressed = jnp.concatenate(parts, axis=0)
        sent[...] = compressed
        piece = compressed.astype(F32)
        out_p[0, :, cols] = stepped
        out_e[0, :, cols] = old + piece
        out_m[0, :, cols] = m_v[:, cols] + w_self * piece

    def mix(cols, left, right):
        mixed = out_m[0, :, cols] + w_left * left[...].astype(F32)
        mixed = mixed + w_right * right[...].astype(F32)
        out_m[0, :, cols] = mixed
        out_p[0, :, cols] = out_p[0, :, cols] + mixing_rate * (mixed - out_e[0, :, cols])

    def slim_mix(k):
        for side in range(2):
            copy_g(side, k).wait_recv()
        mix(aligned(k * cw, cw), g_dst.at[0, k], g_dst.at[1, k])

    def wide_mix(i):
        for side in range(2):
            copy_h(side, i).wait_recv()
        mix(aligned(slim * cw + i * pw, pw), h_dst.at[0, i], h_dst.at[1, i])

    transpose_a(0, 4)
    lax.fori_loop(0, HEAD, multiply_head, 0)
    pl.semaphore_wait(barrier, 6)
    for k in range(HEAD):
        copy_head(k).start()
    transpose_a(4, 16)
    for k in range(HEAD):
        head_first(k)
    lax.fori_loop(0, HEAD, multiply_rest, 0)
    for copy in state:
        copy.wait()

    def drain_slim(k, _):
        copy_x(k).wait_send()
        for side in range(2):
            copy_s1(side, k).wait_send()
            for xd in range(2):
                copy_s2(side, xd, k).wait_send()
        return 0

    def drain_wide(i, _):
        copy_wide(i).wait_send()
        for side in range(2):
            copy_w1(side, i).wait_send()
            for half in range(2):
                copy_w2(side, half, i).wait_send()
        return 0

    def drain_head(k, _):
        copy_head(k).wait_send()
        copy_rest(k).wait_send()
        return 0

    def drain(k, _):
        copy_d(k).wait_send()
        return 0

    def drain_early():
        lax.fori_loop(0, slim, drain_slim, 0)
        lax.fori_loop(0, pieces, drain_wide, 0)
        lax.fori_loop(0, HEAD, drain_head, 0)
        lax.fori_loop(HEAD, chunks, drain, 0)

    def step(t, _):
        for stage, lag, count in (
            (head_direct, 0, HEAD),
            (slim_first, HEAD, slim - HEAD),
            (slim_relay, 1, slim),
            (lambda i: slim_multiply(i + HEAD), 1, slim - HEAD),
            (wide_multiply, 0, wide),
            (wide_first, 1, wide),
            (wide_line, 4, pieces),
            (wide_relay, 6, pieces),
            (slim_cross, 3, slim),
            (wide_finish, 8, pieces),
            (slim_finish, 4, slim),
            (lambda i: drain_early(), pieces + 8, 1),
            (slim_mix, 7, slim),
            (wide_mix, 11, pieces),
        ):
            pl.when((t >= lag) & (t < count + lag))(functools.partial(stage, t - lag))
        return 0

    lax.fori_loop(0, 15, step, 0)

    def drain_slim_cycle(k, _):
        for side in range(2):
            copy_g(side, k).wait_send()
        return 0

    def drain_wide_cycle(i, _):
        for side in range(2):
            copy_h(side, i).wait_send()
        return 0

    lax.fori_loop(0, slim, drain_slim_cycle, 0)
    lax.fori_loop(0, pieces, drain_wide_cycle, 0)


def store(in_p, in_e, in_m, out_p, out_e, out_m, sems):
    copies = [
        pltpu.make_async_copy(src, dst, sems.at[i])
        for i, (src, dst) in enumerate(((in_p, out_p), (in_e, out_e), (in_m, out_m)))
    ]
    for copy in copies:
        copy.start()
    for copy in copies:
        copy.wait()


def on_device(params, estimate, mixed_sum, activations, out_grads, exponents, edge_weight):
    members = lax.axis_size("mem")
    tokens, width = out_grads.shape
    factor = step_size / math.sqrt(members * tokens)
    n = CHUNKS
    cw = width // n
    w = WIDE
    r = n - w
    p = w * cw // 128
    block = (128, cw)
    piece = (128, 128)
    half = (64, 128)
    shard = jax.ShapeDtypeStruct(params.shape, F32)
    anywhere = pl.BlockSpec(memory_space=pl.ANY)
    hbm = pl.BlockSpec(memory_space=pltpu.HBM)
    vmem = pl.BlockSpec(memory_space=pltpu.VMEM)
    dma = pltpu.SemaphoreType.DMA
    exponents = pltpu.with_memory_space_constraint(exponents, pltpu.HBM)
    edge_weight = pltpu.with_memory_space_constraint(edge_weight, pltpu.HBM)
    results = pl.pallas_call(
        functools.partial(kernel, factor),
        out_shape=(shard, shard, shard),
        in_specs=[hbm] * 7,
        out_specs=(vmem, vmem, vmem),
        scratch_shapes=[
            pltpu.VMEM((16, tokens, 128), BF16),
            pltpu.VMEM((n, tokens, cw), BF16),
            pltpu.VMEM((2048, tokens), BF16),
            pltpu.VMEM((128, width), F32),
            pltpu.VMEM((128, width), F32),
            pltpu.VMEM((128, width), F32),
            pltpu.VMEM((2 + w, 1024, cw), F32),
            pltpu.VMEM((n, 1024, cw), BF16),
            pltpu.VMEM((n, 1024, cw), BF16),
            pltpu.VMEM((2, r) + block, F32),
            pltpu.VMEM((2, r) + block, F32),
            pltpu.VMEM((2, r) + block, BF16),
            pltpu.VMEM((2, r) + block, BF16),
            pltpu.VMEM((2, 2, r) + block, BF16),
            pltpu.VMEM((2, 2, r) + block, BF16),
            pltpu.VMEM((r,) + block, BF16),
            pltpu.VMEM((r,) + block, BF16),
            pltpu.VMEM((p, 4) + piece, F32),
            pltpu.VMEM((p, 4) + piece, BF16),
            pltpu.VMEM((p, 4) + piece, BF16),
            pltpu.VMEM((2, p) + half, F32),
            pltpu.VMEM((2, p) + half, F32),
            pltpu.VMEM((2, p) + half, BF16),
            pltpu.VMEM((2, p) + half, BF16),
            pltpu.VMEM((2, 2, p) + half, BF16),
            pltpu.VMEM((2, 2, p) + half, BF16),
            pltpu.VMEM((r,) + block, BF16),
            pltpu.VMEM((2, r) + block, BF16),
            pltpu.VMEM((p,) + piece, BF16),
            pltpu.VMEM((2, p) + piece, BF16),
            pltpu.SMEM((1, 2), jnp.int32),
            pltpu.SMEM((8,), F32),
            dma((16,)),
            dma((n,)),
            dma((5,)),
            dma((2, n)),
            dma((2, HEAD)),
            dma((2, 2, r)),
            dma((2, 2, 2, r)),
            dma((2, r)),
            dma((2, p)),
            dma((2, 2, p)),
            dma((2, 2, 2, p)),
            dma((2, 2, r)),
            dma((2, 2, p)),
        ],
        compiler_params=pltpu.CompilerParams(
            collective_id=0, has_side_effects=True, vmem_limit_bytes=50 * 2**20
        ),
        name="round",
    )(params, estimate, mixed_sum, activations, out_grads, exponents, edge_weight)
    return pl.pallas_call(
        store,
        out_shape=(shard, shard, shard),
        in_specs=[vmem] * 3,
        out_specs=(anywhere,) * 3,
        scratch_shapes=[dma((3,))],
        compiler_params=pltpu.CompilerParams(vmem_limit_bytes=2**20),
        name="store",
    )(*results)


def solution(mesh):
    in_specs = (
        P("grp", "mem", None),
        P("grp", "mem", None),
        P("grp", "mem", None),
        P(("grp", "mem"), None),
        P(("grp", "mem"), None),
        P("grp", "mem"),
        P(),
    )
    out_specs = (P("grp", "mem", None), P("grp", "mem", None), P("grp", "mem", None))
    return jax.shard_map(
        on_device, mesh=mesh, in_specs=in_specs, out_specs=out_specs, check_vma=False
    )
```

```python
import functools
import math

import jax
import jax.numpy as jnp
from jax import lax
from jax.experimental import pallas as pl
from jax.experimental.pallas import tpu as pltpu
from jax.sharding import PartitionSpec as P

step_size = 0.5
mixing_rate = 0.4

MESH = pl.DeviceIdType.MESH
F32 = jnp.float32
BF16 = jnp.bfloat16
CHUNKS = 8
WIDE = 2
HEAD = 2


def aligned(start, size):
    return pl.ds(pl.multiple_of(start, size), size)


def kernel(
    factor,
    params,
    estimate,
    mixed_sum,
    acts,
    grads,
    exponents,
    edge_weight,
    out_p,
    out_e,
    out_m,
    a_v,
    b_v,
    at_v,
    p_v,
    e_v,
    m_v,
    own_v,
    d_src,
    d_dst,
    near_v,
    home_v,
    s1_src,
    s1_dst,
    s2_src,
    s2_dst,
    x_src,
    x_dst,
    wide_own,
    wide_src,
    wide_dst,
    near_w,
    home_w,
    w1_src,
    w1_dst,
    w2_src,
    w2_dst,
    g_src,
    g_dst,
    h_src,
    h_dst,
    powers,
    weights,
    a_sem,
    b_sem,
    l_sem,
    d_sem,
    head_sem,
    s1_sem,
    s2_sem,
    x_sem,
    wide_sem,
    w1_sem,
    w2_sem,
    g_sem,
    h_sem,
):
    g = lax.axis_index("grp")
    m = lax.axis_index("mem")
    z = m // 4
    x = (m // 2) % 2
    c = m % 2
    pc = 1 - c
    zp, zm, zo = (z + 1) % 4, (z + 3) % 4, (z + 2) % 4
    to_core = (g, z * 4 + x * 2 + pc)
    to_line = ((g, zp * 4 + x * 2 + c), (g, zm * 4 + x * 2 + c))
    to_x = (g, z * 4 + (1 - x) * 2 + c)
    to_cycle = (((g + 1) % 8, m), ((g + 7) % 8, m))
    chunks, _, cw = b_v.shape
    pieces, _, _, pw = wide_src.shape
    wide = pieces * pw // cw
    slim = chunks - wide
    line = (zo, zp, zm, z)

    barrier = pltpu.get_barrier_semaphore()
    for peer in (to_core, to_x) + to_line + to_cycle:
        pl.semaphore_signal(barrier, inc=1, device_id=peer, device_id_type=MESH)

    def load_a(i, slot):
        j, xd, par = i
        block = line[j] * 4 + xd * 2 + (pc, c)[par]
        return pltpu.make_async_copy(
            acts.at[:, aligned(block * 128, 128)], a_v.at[slot], a_sem.at[slot]
        )

    def load_b(k):
        return pltpu.make_async_copy(grads.at[:, aligned(k * cw, cw)], b_v.at[k], b_sem.at[k])

    blocks = [(0, xd, par) for par in range(2) for xd in range(2)]
    blocks += [(j, xd, par) for par in range(2) for j in range(1, 4) for xd in range(2)]
    for slot, i in enumerate(blocks):
        if slot == 4:
            for k in range(HEAD):
                load_b(k).start()
        load_a(i, slot).start()
    small = [
        pltpu.make_async_copy(exponents, powers, l_sem.at[3]),
        pltpu.make_async_copy(edge_weight, weights, l_sem.at[4]),
    ]
    state = [
        pltpu.make_async_copy(src.at[0], dst, l_sem.at[i])
        for i, (src, dst) in enumerate(((params, p_v), (estimate, e_v), (mixed_sum, m_v)))
    ]
    for k in (slim, HEAD, *range(slim + 1, chunks), *range(HEAD + 1, slim)):
        load_b(k).start()
    for copy in small + state:
        copy.start()

    def transpose_a(low, high):
        def body(slot, _):
            pltpu.make_async_copy(
                acts.at[:, pl.ds(0, 128)], a_v.at[slot], a_sem.at[slot]
            ).wait()
            at_v[aligned(slot * 128, 128), :] = a_v[slot].T
            return 0

        lax.fori_loop(low, high, body, 0)

    def remote(src, dst, sems, index, peer):
        return pltpu.make_async_remote_copy(
            src_ref=src,
            dst_ref=dst,
            send_sem=sems.at[(0,) + index],
            recv_sem=sems.at[(1,) + index],
            device_id=peer,
            device_id_type=MESH,
        )

    def copy_d(k):
        return remote(d_src.at[k], d_dst.at[k], d_sem, (k,), to_core)

    def copy_head(k):
        rows = pl.ds(0, 256)
        return remote(d_src.at[k, rows], d_dst.at[k, rows], head_sem, (k,), to_core)

    def copy_rest(k):
        rows = pl.ds(256, 768)
        return remote(d_src.at[k, rows], d_dst.at[k, rows], d_sem, (k,), to_core)

    def copy_s1(side, k):
        return remote(
            s1_src.at[side, k], s1_dst.at[side, k], s1_sem, (side, k), to_line[side]
        )

    def copy_s2(side, xd, k):
        return remote(
            s2_src.at[side, xd, k],
            s2_dst.at[side, xd, k],
            s2_sem,
            (side, xd, k),
            to_line[side],
        )

    def copy_x(k):
        return remote(x_src.at[k], x_dst.at[k], x_sem, (k,), to_x)

    def copy_wide(i):
        return remote(wide_src.at[i], wide_dst.at[i], wide_sem, (i,), to_x)

    def copy_w1(side, i):
        return remote(
            w1_src.at[side, i], w1_dst.at[side, i], w1_sem, (side, i), to_line[side]
        )

    def copy_w2(side, half, i):
        return remote(
            w2_src.at[side, half, i],
            w2_dst.at[side, half, i],
            w2_sem,
            (side, half, i),
            to_line[side],
        )

    def copy_g(side, k):
        return remote(
            g_src.at[k], g_dst.at[side, k], g_sem, (side, k), to_cycle[side]
        )

    def copy_h(side, i):
        return remote(
            h_src.at[i], h_dst.at[side, i], h_sem, (side, i), to_cycle[side]
        )

    def multiply(k, slot):
        load_b(k).wait()
        both = jnp.dot(at_v[...], b_v[k], preferred_element_type=F32)
        d_src[k, pl.ds(0, 256), :] = both[:256].astype(BF16)
        own_v[slot, pl.ds(0, 256), :] = both[256:512]
        d_src[k, pl.ds(256, 768), :] = both[512:1280].astype(BF16)
        own_v[slot, pl.ds(256, 768), :] = both[1280:]
        copy_d(k).start()

    def multiply_head(k, _):
        load_b(k).wait()
        both = jnp.dot(at_v[pl.ds(0, 512), :], b_v[k], preferred_element_type=F32)
        d_src[k, pl.ds(0, 256), :] = both[:256].astype(BF16)
        own_v[k, pl.ds(0, 256), :] = both[256:]
        return 0

    def multiply_rest(k, _):
        both = jnp.dot(at_v[pl.ds(512, 1536), :], b_v[k], preferred_element_type=F32)
        d_src[k, pl.ds(256, 768), :] = both[:768].astype(BF16)
        own_v[k, pl.ds(256, 768), :] = both[768:]
        copy_rest(k).start()
        return 0

    def slim_multiply(k):
        multiply(k, k % 2)

    def wide_multiply(i):
        multiply(slim + i, 2 + i)

    def chip_sum(k, slot, j, xd):
        rows = aligned((j * 2 + xd) * 128, 128)
        return own_v[slot, rows, :] + d_dst[k, rows, :].astype(F32)

    def send_first(k):
        for side in range(2):
            s1_src[side, k] = chip_sum(k, k % 2, 0, side).astype(BF16)
            copy_s1(side, k).start()

    def send_direct(k):
        part = functools.partial(chip_sum, k, k % 2)
        for side in range(2):
            s2_src[side, 1 - side, k] = part(1 + side, 1 - side).astype(BF16)
            copy_s2(side, 1 - side, k).start()
        for side in range(2):
            near_v[side, k] = part(1 + side, side)
        for xd in range(2):
            home_v[xd, k] = part(3, xd)

    def head_first(k):
        copy_head(k).wait_recv()
        send_first(k)

    def head_direct(k):
        copy_rest(k).wait_recv()
        send_direct(k)

    def slim_first(k):
        k = k + HEAD
        copy_d(k).wait_recv()
        send_first(k)
        send_direct(k)

    def slim_relay(k):
        for side in range(2):
            copy_s1(side, k).wait_recv()
            s2_src[side, side, k] = (near_v[side, k] + s1_dst[side, k].astype(F32)).astype(BF16)
            copy_s2(side, side, k).start()

    def slim_cross(k):
        for side in range(2):
            for xd in range(2):
                copy_s2(side, xd, k).wait_recv()

        def line_sum(xd):
            return home_v[xd, k] + s2_dst[0, xd, k].astype(F32) + s2_dst[1, xd, k].astype(F32)

        x_src[k] = line_sum(1 - x).astype(BF16)
        copy_x(k).start()
        home_v[x, k] = line_sum(x)

    def slim_finish(k):
        copy_x(k).wait_recv()
        compress(aligned(k * cw, cw), home_v[x, k] + x_dst[k].astype(F32), g_src.at[k])
        for side in range(2):
            copy_g(side, k).start()

    def wide_first(i):
        k = slim + i
        copy_d(k).wait_recv()
        for j in range(4):
            away = chip_sum(k, 2 + i, j, 1 - x).astype(BF16)
            for part in range(cw // pw):
                wide_src[i * (cw // pw) + part, j] = away[:, part * pw : (part + 1) * pw]
        for part in range(cw // pw):
            copy_wide(i * (cw // pw) + part).start()
        for j in range(4):
            keep = chip_sum(k, 2 + i, j, x)
            for part in range(cw // pw):
                wide_own[i * (cw // pw) + part, j] = keep[:, part * pw : (part + 1) * pw]

    def wide_line(i):
        copy_wide(i).wait_recv()

        def pair_sum(j, half):
            rows = pl.ds(half * 64, 64)
            return wide_own[i, j, rows, :] + wide_dst[i, j, rows, :].astype(F32)

        for side in range(2):
            w1_src[side, i] = pair_sum(0, side).astype(BF16)
            copy_w1(side, i).start()
        for side in range(2):
            w2_src[side, 1 - side, i] = pair_sum(1 + side, 1 - side).astype(BF16)
            copy_w2(side, 1 - side, i).start()
        for side in range(2):
            near_w[side, i] = pair_sum(1 + side, side)
        for half in range(2):
            home_w[half, i] = pair_sum(3, half)

    def wide_relay(i):
        for side in range(2):
            copy_w1(side, i).wait_recv()
            w2_src[side, side, i] = (near_w[side, i] + w1_dst[side, i].astype(F32)).astype(BF16)
            copy_w2(side, side, i).start()

    def wide_finish(i):
        for side in range(2):
            for half in range(2):
                copy_w2(side, half, i).wait_recv()
        sums = [
            home_w[half, i] + w2_dst[0, half, i].astype(F32) + w2_dst[1, half, i].astype(F32)
            for half in range(2)
        ]
        start = slim * cw + i * pw
        compress(aligned(start, pw), jnp.concatenate(sums, axis=0), h_src.at[i])
        for side in range(2):
            copy_h(side, i).start()

    for copy in small:
        copy.wait()
    w_right = weights[g]
    w_left = weights[(g + 7) % 8]
    w_self = 1.0 - w_left - w_right

    def compress(cols, gradient, sent):
        old = e_v[:, cols]
        stepped = p_v[:, cols] - factor * gradient
        change = stepped - old
        parts = []
        for i in range(2):
            scale = lax.shift_left(1, powers[0, i]).astype(F32)
            scale = jnp.full((64, change.shape[1]), scale, F32)
            levels = jnp.clip(change[i * 64 : (i + 1) * 64] / scale, -1.0, 1.0).astype(BF16)
            parts.append((levels.astype(F32) * scale).astype(BF16))
        compressed = jnp.concatenate(parts, axis=0)
        sent[...] = compressed
        piece = compressed.astype(F32)
        out_p[0, :, cols] = stepped
        out_e[0, :, cols] = old + piece
        out_m[0, :, cols] = m_v[:, cols] + w_self * piece

    def mix(cols, left, right):
        mixed = out_m[0, :, cols] + w_left * left[...].astype(F32)
        mixed = mixed + w_right * right[...].astype(F32)
        out_m[0, :, cols] = mixed
        out_p[0, :, cols] = out_p[0, :, cols] + mixing_rate * (mixed - out_e[0, :, cols])

    def slim_mix(k):
        for side in range(2):
            copy_g(side, k).wait_recv()
        mix(aligned(k * cw, cw), g_dst.at[0, k], g_dst.at[1, k])

    def wide_mix(i):
        for side in range(2):
            copy_h(side, i).wait_recv()
        mix(aligned(slim * cw + i * pw, pw), h_dst.at[0, i], h_dst.at[1, i])

    transpose_a(0, 4)
    lax.fori_loop(0, HEAD, multiply_head, 0)
    pl.semaphore_wait(barrier, 6)
    for k in range(HEAD):
        copy_head(k).start()
    transpose_a(4, 16)
    for k in range(HEAD):
        head_first(k)
    lax.fori_loop(0, HEAD, multiply_rest, 0)
    for copy in state:
        copy.wait()

    def drain_slim(k, _):
        copy_x(k).wait_send()
        for side in range(2):
            copy_s1(side, k).wait_send()
            for xd in range(2):
                copy_s2(side, xd, k).wait_send()
        return 0

    def drain_wide(i, _):
        copy_wide(i).wait_send()
        for side in range(2):
            copy_w1(side, i).wait_send()
            for half in range(2):
                copy_w2(side, half, i).wait_send()
        return 0

    def drain_head(k, _):
        copy_head(k).wait_send()
        copy_rest(k).wait_send()
        return 0

    def drain(k, _):
        copy_d(k).wait_send()
        return 0

    def drain_early():
        lax.fori_loop(0, slim, drain_slim, 0)
        lax.fori_loop(0, pieces, drain_wide, 0)
        lax.fori_loop(0, HEAD, drain_head, 0)
        lax.fori_loop(HEAD, chunks, drain, 0)

    def step(t, _):
        for stage, lag, count in (
            (head_direct, 0, HEAD),
            (slim_first, HEAD, slim - HEAD),
            (slim_relay, 1, slim),
            (lambda i: slim_multiply(i + HEAD), 1, slim - HEAD),
            (slim_cross, 3, slim),
            (wide_multiply, 0, wide),
            (wide_first, 1, wide),
            (wide_line, 4, pieces),
            (wide_relay, 6, pieces),
            (wide_finish, 8, pieces),
            (slim_finish, 4, slim),
            (lambda i: drain_early(), pieces + 8, 1),
            (slim_mix, 7, slim),
            (wide_mix, 11, pieces),
        ):
            pl.when((t >= lag) & (t < count + lag))(functools.partial(stage, t - lag))
        return 0

    lax.fori_loop(0, 15, step, 0)

    def drain_slim_cycle(k, _):
        for side in range(2):
            copy_g(side, k).wait_send()
        return 0

    def drain_wide_cycle(i, _):
        for side in range(2):
            copy_h(side, i).wait_send()
        return 0

    lax.fori_loop(0, slim, drain_slim_cycle, 0)
    lax.fori_loop(0, pieces, drain_wide_cycle, 0)


def store(in_p, in_e, in_m, out_p, out_e, out_m, sems):
    copies = [
        pltpu.make_async_copy(src, dst, sems.at[i])
        for i, (src, dst) in enumerate(((in_p, out_p), (in_e, out_e), (in_m, out_m)))
    ]
    for copy in copies:
        copy.start()
    for copy in copies:
        copy.wait()


def on_device(params, estimate, mixed_sum, activations, out_grads, exponents, edge_weight):
    members = lax.axis_size("mem")
    tokens, width = out_grads.shape
    factor = step_size / math.sqrt(members * tokens)
    n = CHUNKS
    cw = width // n
    w = WIDE
    r = n - w
    p = w * cw // 128
    block = (128, cw)
    piece = (128, 128)
    half = (64, 128)
    shard = jax.ShapeDtypeStruct(params.shape, F32)
    anywhere = pl.BlockSpec(memory_space=pl.ANY)
    hbm = pl.BlockSpec(memory_space=pltpu.HBM)
    vmem = pl.BlockSpec(memory_space=pltpu.VMEM)
    dma = pltpu.SemaphoreType.DMA
    exponents = pltpu.with_memory_space_constraint(exponents, pltpu.HBM)
    edge_weight = pltpu.with_memory_space_constraint(edge_weight, pltpu.HBM)
    results = pl.pallas_call(
        functools.partial(kernel, factor),
        out_shape=(shard, shard, shard),
        in_specs=[hbm] * 7,
        out_specs=(vmem, vmem, vmem),
        scratch_shapes=[
            pltpu.VMEM((16, tokens, 128), BF16),
            pltpu.VMEM((n, tokens, cw), BF16),
            pltpu.VMEM((2048, tokens), BF16),
            pltpu.VMEM((128, width), F32),
            pltpu.VMEM((128, width), F32),
            pltpu.VMEM((128, width), F32),
            pltpu.VMEM((2 + w, 1024, cw), F32),
            pltpu.VMEM((n, 1024, cw), BF16),
            pltpu.VMEM((n, 1024, cw), BF16),
            pltpu.VMEM((2, r) + block, F32),
            pltpu.VMEM((2, r) + block, F32),
            pltpu.VMEM((2, r) + block, BF16),
            pltpu.VMEM((2, r) + block, BF16),
            pltpu.VMEM((2, 2, r) + block, BF16),
            pltpu.VMEM((2, 2, r) + block, BF16),
            pltpu.VMEM((r,) + block, BF16),
            pltpu.VMEM((r,) + block, BF16),
            pltpu.VMEM((p, 4) + piece, F32),
            pltpu.VMEM((p, 4) + piece, BF16),
            pltpu.VMEM((p, 4) + piece, BF16),
            pltpu.VMEM((2, p) + half, F32),
            pltpu.VMEM((2, p) + half, F32),
            pltpu.VMEM((2, p) + half, BF16),
            pltpu.VMEM((2, p) + half, BF16),
            pltpu.VMEM((2, 2, p) + half, BF16),
            pltpu.VMEM((2, 2, p) + half, BF16),
            pltpu.VMEM((r,) + block, BF16),
            pltpu.VMEM((2, r) + block, BF16),
            pltpu.VMEM((p,) + piece, BF16),
            pltpu.VMEM((2, p) + piece, BF16),
            pltpu.SMEM((1, 2), jnp.int32),
            pltpu.SMEM((8,), F32),
            dma((16,)),
            dma((n,)),
            dma((5,)),
            dma((2, n)),
            dma((2, HEAD)),
            dma((2, 2, r)),
            dma((2, 2, 2, r)),
            dma((2, r)),
            dma((2, p)),
            dma((2, 2, p)),
            dma((2, 2, 2, p)),
            dma((2, 2, r)),
            dma((2, 2, p)),
        ],
        compiler_params=pltpu.CompilerParams(
            collective_id=0, has_side_effects=True, vmem_limit_bytes=50 * 2**20
        ),
        name="round",
    )(params, estimate, mixed_sum, activations, out_grads, exponents, edge_weight)
    return pl.pallas_call(
        store,
        out_shape=(shard, shard, shard),
        in_specs=[vmem] * 3,
        out_specs=(anywhere,) * 3,
        scratch_shapes=[dma((3,))],
        compiler_params=pltpu.CompilerParams(vmem_limit_bytes=2**20),
        name="store",
    )(*results)


def solution(mesh):
    in_specs = (
        P("grp", "mem", None),
        P("grp", "mem", None),
        P("grp", "mem", None),
        P(("grp", "mem"), None),
        P(("grp", "mem"), None),
        P("grp", "mem"),
        P(),
    )
    out_specs = (P("grp", "mem", None), P("grp", "mem", None), P("grp", "mem", None))
    return jax.shard_map(
        on_device, mesh=mesh, in_specs=in_specs, out_specs=out_specs, check_vma=False
    )
```
